32 devices in a mesh: rows: 8 (over z, y), mem: 4 (over x, core).
Axes of the slice: x: 2, y: 2, z: 4, core: 2. Of those that a mesh axis runs over, the one named last changes fastest.
Arguments:
- control: bfloat16 [16, 32, 2, 512, 512], P('mem', None, None, 'rows'), may hold values from -6 to 6
- vert_root: float32 [32, 32], replicated, may hold values from -1 to 1
- loc_spec: float32 [512], replicated, may hold values from 0.1 to 1
- legendre: bfloat16 [512, 512, 768], P('rows'), as said below
- wave_table: int32 [512], replicated, may hold values from 0 to 511, as said below
- lat_order: int32 [768], replicated, may hold values from 0 to 767, each once
- perturb: bfloat16 [768, 16, 32, 1536], P('rows', None, 'mem'), may hold values from -3 to 3
Outputs:
- increment: bfloat16 [768, 32, 1536], P('rows', 'mem')
The draws below stay inside these ranges and needn't reach their ends.
Inputs may be any that keep to these rules, and one draw needn't show every extreme that they name: `wave_table`: every zonal wavenumber 0 to 511 sits in exactly one slot; the slots held by one index of rows are pairs m and 511 - m. legendre[s, n, t] is zero where n < wave_table[s]. `lat_order`: a permutation.
All inputs are finite; a program needn't handle non-finite values.
Results may differ from the reference program's by a relative error of at most 0.0085.
Values may be sent and summed in bfloat16 or wider, within the bound.
A program may use at most 256 MiB of HBM per device.

```python
import math
import jax
import jax.numpy as jnp
from jax import lax

NM = 512
NT = 512
NLAT = 768
NLON = 1536
MEMBERS = 16
LEV = 32
N_ROWS = 8


def pair_table(key):
    subkey = jax.random.fold_in(key, 7)
    permuted = jax.random.permutation(subkey, NM // 2).astype(jnp.int32)
    lower_half = permuted.reshape(N_ROWS, NM // (2 * N_ROWS))
    return jnp.concatenate([lower_half, NM - 1 - lower_half], axis=1).reshape(NM).astype(jnp.int32)


def draw_wave_table(key, part):
    return pair_table(key)


def draw_legendre(key, part):
    table = pair_table(key)
    subkey = jax.random.fold_in(key, 11)
    values = jax.random.normal(subkey, (NM, NT, NLAT), jnp.float32)
    totals = jnp.arange(NT, dtype=jnp.int32)
    triangle = (totals[None, :] >= table[:, None]).astype(jnp.float32)
    factor = (4.0 * NM * NT) ** (-0.5)
    return (values * factor * triangle[:, :, None]).astype(jnp.bfloat16)


def block_levels(key, extent, split, low, top_value):
    level = 1.0
    for dim, shards_of in split:
        draws = jax.random.uniform(jax.random.fold_in(jax.random.fold_in(key, 6), dim), (shards_of,), jnp.float32, low / len(split), top_value / len(split))
        level = level * jnp.repeat(jnp.exp(draws), extent[dim] // shards_of).reshape((-1,) + (1,) * (len(extent) - 1 - dim))
    return level


def noise(rng, dims, spread, reach, pieces=(), held_as=jnp.bfloat16):
    gain = block_levels(rng, dims, pieces, -0.22, 0.18) if pieces else 1.0
    values = jax.random.normal(rng, dims, jnp.float32) * spread * gain
    return jnp.minimum(jnp.maximum(values, -reach), reach).astype(held_as)


def setup_inputs(seed: int = 0) -> dict:
    key_list = jax.random.split(jax.random.key(seed), 8)
    control = noise(key_list[0], (MEMBERS, LEV, 2, NM, NT), 1.0, 6.0, ((0, 4), (3, 8)))
    vert_root = noise(key_list[1], (LEV, LEV), LEV ** -0.5, 1.0, (), jnp.float32)
    loc_spec = jnp.clip(jnp.exp(jax.random.uniform(key_list[2], (NT,), jnp.float32, math.log(0.1), math.log(1.0))), 0.1, 1.0)
    legendre = draw_legendre(jax.random.fold_in(key_list[7], 71), 0)
    wave_table = draw_wave_table(jax.random.fold_in(key_list[7], 71), 0)
    lat_order = jax.random.permutation(key_list[5], NLAT).astype(jnp.int32)
    perturb = noise(key_list[6], (NLAT, MEMBERS, LEV, NLON), 0.5, 3.0, ((0, 8), (2, 4)))
    return {"control": control, "vert_root": vert_root, "loc_spec": loc_spec, "legendre": legendre, "wave_table": wave_table, "lat_order": lat_order, "perturb": perturb}


def make_basis(wave_table, lon_count):
    longitude = lax.iota(jnp.int32, lon_count)
    phases = (wave_table[:, None] * longitude[None, :]) % lon_count
    angles = phases.astype(jnp.float32) * (2.0 * math.pi / lon_count)
    weights = jnp.where(wave_table == 0, 1.0, 2.0).astype(jnp.float32)[:, None]
    return jnp.stack([weights * jnp.cos(angles), -weights * jnp.sin(angles)]).astype(jnp.bfloat16)


def reference(control, vert_root, loc_spec, legendre, wave_table, lat_order, perturb):
    scaled = control.astype(jnp.float32) * loc_spec
    spectra = jnp.einsum('lv,kvrsn->klrsn', vert_root, scaled, precision=lax.Precision.HIGHEST).astype(jnp.bfloat16)
    zonal_basis = make_basis(wave_table, NLON).astype(jnp.float32)
    legendre_wide = legendre.astype(jnp.float32)

    def one_level(level_index):
        level_spec = lax.dynamic_index_in_dim(spectra, level_index, 1, keepdims=False).astype(jnp.float32)
        fourier = jnp.einsum('snt,krsn->strk', legendre_wide, level_spec, precision=lax.Precision.HIGHEST).astype(jnp.bfloat16)
        fourier = jnp.take(fourier, lat_order, axis=1).astype(jnp.float32)
        fields = jnp.einsum('sjrk,rsx->jkx', fourier, zonal_basis, precision=lax.Precision.HIGHEST).astype(jnp.bfloat16)
        member_ptb = lax.dynamic_index_in_dim(perturb, level_index, 2, keepdims=False).astype(jnp.float32)
        return jnp.sum(fields.astype(jnp.float32) * member_ptb, axis=1).astype(jnp.bfloat16)

    stacked = lax.map(one_level, jnp.arange(LEV, dtype=jnp.int32))
    return jnp.transpose(stacked, (1, 0, 2))
```

```python
import functools
import math

import jax
import jax.numpy as jnp
from jax import lax
from jax.experimental import pallas as pl
from jax.experimental.pallas import tpu as pltpu
from jax.sharding import PartitionSpec as P

HALVES = 2
LATS = 4
VMEM_LIMIT = 56 * 1024 * 1024


def make_basis(wave_table, lon_count):
    longitude = lax.iota(jnp.int32, lon_count)
    phases = wave_table[:, None] * longitude[None, :] % lon_count
    angles = phases.astype(jnp.float32) * (2.0 * math.pi / lon_count)
    weights = jnp.where(wave_table == 0, 1.0, 2.0).astype(jnp.float32)[:, None]
    return jnp.stack([weights * jnp.cos(angles), -weights * jnp.sin(angles)]).astype(jnp.bfloat16)


def legendre_kernel(*refs):
    specs, (leg_ref, order_ref, out_ref) = refs[:-3], refs[-3:]
    members, parts, _, levels, totals = specs[0].shape
    rows = [
        s[:, r, 0].reshape(members * levels, totals) for r in range(parts) for s in specs
    ]
    spec = jnp.concatenate(rows, axis=0)
    fourier = jnp.dot(spec, leg_ref[0], preferred_element_type=jnp.float32).astype(jnp.bfloat16)
    stored = lax.dot_general(
        order_ref[...], fourier, (((1,), (1,)), ((), ())), preferred_element_type=jnp.float32
    ).astype(jnp.bfloat16)
    lats = out_ref.shape[2]
    for d in range(out_ref.shape[0]):
        out_ref[d, 0] = stored[d * lats : (d + 1) * lats]


def legendre_step(specs, legendre, order, first, row_count):
    members, parts, slots, levels, totals = specs[0].shape
    lat_count = legendre.shape[2]
    lats = lat_count // row_count
    width = len(specs) * members * parts * levels
    flops = 2 * slots * width * lat_count * (totals + lat_count)
    return pl.pallas_call(
        legendre_kernel,
        grid=(slots,),
        out_shape=jax.ShapeDtypeStruct((row_count, slots, lats, width), jnp.bfloat16),
        in_specs=[
            pl.BlockSpec((members, parts, 1, levels, totals), lambda s: (0, 0, s, 0, 0))
            for _ in specs
        ]
        + [
            pl.BlockSpec((1, totals, lat_count), lambda s: (first + s, 0, 0)),
            pl.BlockSpec((lat_count, lat_count), lambda s: (0, 0)),
        ],
        out_specs=pl.BlockSpec((row_count, 1, lats, width), lambda s: (0, s, 0, 0)),
        compiler_params=pltpu.CompilerParams(vmem_limit_bytes=VMEM_LIMIT),
        cost_estimate=pl.CostEstimate(
            flops=flops,
            bytes_accessed=2 * slots * (totals + width) * lat_count,
            transcendentals=0,
        ),
    )(*specs, legendre, order)


def zonal_kernel(chunks, half, *refs):
    fours, (basis_ref, ptb_ref, before_ref, out_ref) = refs[:chunks], refs[chunks:]
    lats, members, levels, lon_count = ptb_ref.shape
    mem_count = lax.axis_size("mem")
    me = lax.axis_index("mem")
    share = members // mem_count
    taken = share // HALVES
    width = fours[0].shape[2] // 2
    blocks = []
    for j in range(lats):
        pairs = [f[j].T for f in fours]
        blocks.append(
            jnp.concatenate([p[r * width : (r + 1) * width] for p in pairs for r in range(2)], axis=1)
        )
    lhs = jnp.concatenate(blocks, axis=0)
    piece = 512 if lon_count % 512 == 0 else lon_count
    for x in range(0, lon_count, piece):
        field = jnp.dot(lhs, basis_ref[:, x : x + piece], preferred_element_type=jnp.float32)
        field = field.astype(jnp.bfloat16).astype(jnp.float32)
        field = field.reshape(lats, mem_count, taken, levels, piece)
        total = jnp.zeros((lats, levels, piece), jnp.float32)
        if half > 0:
            total = before_ref[:, :, x : x + piece]
        for i in range(mem_count):
            source = lax.rem(me + mem_count - i, mem_count)
            begin = source * share + half * taken
            ptb = ptb_ref[:, pl.ds(begin, taken), :, x : x + piece].astype(jnp.float32)
            total += jnp.sum(field[:, i] * ptb, axis=1)
        out_ref[:, :, x : x + piece] = total.astype(out_ref.dtype)


def zonal_step(fours, basis, perturb, half, before):
    lats, members, levels, lon_count = perturb.shape
    width = fours[0].shape[2]
    depth = basis.shape[0]
    block = math.gcd(LATS, lats)
    out_type = jnp.bfloat16 if half == HALVES - 1 else jnp.float32
    row = pl.BlockSpec((block, levels, lon_count), lambda j: (j, 0, 0))
    kept = row if half > 0 else pl.BlockSpec((1, 8, 128), lambda j: (0, 0, 0))
    return pl.pallas_call(
        functools.partial(zonal_kernel, len(fours), half),
        grid=(lats // block,),
        out_shape=jax.ShapeDtypeStruct((lats, levels, lon_count), out_type),
        in_specs=[
            pl.BlockSpec((block, f.shape[1], width), lambda j: (j, 0, 0)) for f in fours
        ]
        + [
            pl.BlockSpec((depth, lon_count), lambda j: (0, 0)),
            pl.BlockSpec((block, members, levels, lon_count), lambda j: (j, 0, 0, 0)),
            kept,
        ],
        out_specs=row,
        compiler_params=pltpu.CompilerParams(vmem_limit_bytes=VMEM_LIMIT),
        cost_estimate=pl.CostEstimate(
            flops=lats * depth * width * lon_count,
            bytes_accessed=2 * perturb.size,
            transcendentals=0,
        ),
    )(*fours, basis, perturb, before)


def ordered_basis(wave_table, parts, row_count, lon_count):
    table = wave_table.reshape(row_count, -1)
    pieces, first = [], 0
    basis = make_basis(table.reshape(-1), lon_count).reshape(2, row_count, -1, lon_count)
    for slots in parts:
        pieces.append(basis[:, :, first : first + slots].reshape(-1, lon_count))
        first += slots
    return jnp.concatenate(pieces, axis=0)


def shards(control, vert_root, loc_spec, legendre, wave_table, lat_order, perturb):
    mem_count = lax.axis_size("mem")
    row_count = lax.axis_size("rows")
    members, levels, _, slot_count, totals = control.shape
    lat_count = legendre.shape[2]
    share = levels // mem_count
    me = lax.axis_index("mem")
    root = vert_root.reshape(mem_count, share, levels).astype(jnp.bfloat16)
    root = jnp.take(root, (me + lax.iota(jnp.int32, mem_count)) % mem_count, axis=0)
    order = (lat_order[:, None] == lax.iota(jnp.int32, lat_count)[None, :]).astype(jnp.bfloat16)

    taken = members // HALVES
    eighth = slot_count // 8
    splits = [(2 * eighth, 3 * eighth, 3 * eighth), (4 * eighth, 4 * eighth)]
    partial = jnp.zeros((1, 8, 128), jnp.float32)
    for half, split in enumerate(splits):
        fours, first = [], 0
        for slots in split:
            spec = jnp.einsum(
                "dlv,kvrsn->dkrsln",
                root,
                control[half * taken : (half + 1) * taken, :, :, first : first + slots],
                preferred_element_type=jnp.float32,
            )
            spec = (spec * loc_spec).astype(jnp.bfloat16)
            specs = [spec[0]] + [
                lax.ppermute(spec[i], "mem", [(d, (d + i) % mem_count) for d in range(mem_count)])
                for i in range(1, mem_count)
            ]
            four = legendre_step(specs, legendre, order, first, row_count)
            four = lax.all_to_all(four, "rows", split_axis=0, concat_axis=0, tiled=True)
            four = four.reshape(row_count * slots, four.shape[2], four.shape[3]).swapaxes(0, 1)
            fours.append(four)
            first += slots
        basis = ordered_basis(wave_table, split, row_count, perturb.shape[3])
        partial = zonal_step(fours, basis, perturb, half, partial)
    return partial


def solution(mesh):
    return jax.shard_map(
        shards,
        mesh=mesh,
        in_specs=(
            P("mem", None, None, "rows", None),
            P(),
            P(),
            P("rows", None, None),
            P(),
            P(),
            P("rows", None, "mem", None),
        ),
        out_specs=P("rows", "mem", None),
        check_vma=False,
    )
```
